32 devices in a mesh: expert: 16 (over z, y, x), replica: 2 (over core).
Axes of the slice: x: 2, y: 2, z: 4, core: 2. Of those that a mesh axis runs over, the one named last changes fastest.
Arguments:
- tokens: bfloat16 [16384, 1024], P(('expert', 'replica')), may hold values from -6 to 6
- expert_id: int32 [16384, 1], P(('expert', 'replica')), may hold values from 0 to 15; in each aligned block of 512 rows (0 to 511, 512 to 1023, ...) at most 64 rows name the same one
- router_prob: float32 [16384], P(('expert', 'replica')), may hold values from 0.1 to 1
- keep_mask: int32 [16, 32, 2048], P('expert'), may hold values 0 or 1
- w_in: bfloat16 [16, 1024, 2048], P('expert'), may hold values from -0.1875 to 0.1875
- w_out: bfloat16 [16, 2048, 1024], P('expert'), may hold values from -0.125 to 0.125
- cotangent: bfloat16 [16384, 1024], P(('expert', 'replica')), may hold values from -0.59765625 to 0.59765625
Outputs:
- mixed: bfloat16 [16384, 1024], P(('expert', 'replica'))
- grad_in: float32 [16, 1024, 2048], P('expert', 'replica')
- grad_out: float32 [16, 2048, 1024], P('expert', 'replica')
The draws below stay inside these ranges and needn't reach their ends.
Inputs may be any that keep to these rules, and one draw needn't show every extreme that they name: `expert_id`: among the 512 tokens of one device no expert is chosen more than 64 times; on some devices one expert is chosen exactly 64 times.
All inputs are finite; a program needn't handle non-finite values. No bound on the sum of `keep_mask` on one device may be relied on, other than what follows from the above.
Results may differ from the reference program's by a relative error of at most 0.0057.
Values may be sent and summed in bfloat16 or wider, within the bound.
A program may use at most 128 MiB of HBM per device.

```python
import math
import jax
import jax.numpy as jnp
import numpy as np
from jax import lax

D = 1024
FF = 2048
TOK_DEV = 512
EXPERTS = 16
SOURCES = 32
TOKENS = 16384
CAP = 64


def set_ends(result, key, smallest, largest):
    longest = result.shape.index(max(result.shape))
    spots = []
    for shift in (0, 1):
        where = [jax.random.randint(jax.random.fold_in(key, axis), (), 0, length) for axis, length in enumerate(result.shape)]
        where[longest] = (where[longest] + shift) % result.shape[longest]
        spots.append(tuple(where))
    return result.at[spots[0]].set(smallest).at[spots[1]].set(largest)


def level_of(own_key, dims, shards, low, high):
    def one(axis_at, parts):
        steps = jax.random.uniform(jax.random.fold_in(jax.random.fold_in(own_key, 6), axis_at), (parts,), jnp.float32, low / len(shards), high / len(shards))
        return jnp.repeat(jnp.exp(steps), dims[axis_at] // parts).reshape((-1,) + (1,) * (len(dims) - axis_at - 1))

    gain = one(*shards[0])
    for cut in shards[1:]:
        gain = gain * one(*cut)
    return gain


def deal_out(own_key, own, number, rows, count, top, limit, skew):
    ranking = jax.random.permutation(own_key, count)
    packed, common = portions_of(count, rows * top, limit, skew, True), portions_of(count, rows * top, limit, skew, False)
    places = jnp.arange(count)

    def named(sizes, rotation):
        used = int((sizes > 0).sum())
        fixed = max(1, used // 4)
        shifted = fixed + (places - fixed + rotation * (used - fixed)) % max(1, count - fixed)
        return jnp.zeros((count,), jnp.int32).at[ranking[jnp.where(places < fixed, places, shifted)]].set(jnp.asarray(sizes, jnp.int32))

    sizes = jnp.where(number % 4 == 0, named(packed, number // 4), named(common, number - number // 4 - 1))
    mixed = jax.random.permutation(jax.random.fold_in(own, 3), count)
    giver, taker = mixed[0:count // 2 * 2:2], mixed[1:count // 2 * 2:2]
    room = jnp.minimum(sizes[giver] - 1, limit - sizes[taker]) // 2
    room = jnp.where((giver == ranking[0]) | (taker == ranking[0]) | (sizes[taker] == 0), 0, jnp.maximum(room, 0))
    shifted = jax.random.randint(jax.random.fold_in(own, 4), (count // 2,), 0, 1 << 20) % (room + 1)
    sizes = sizes.at[giver].add(-shifted).at[taker].add(shifted)
    items = jnp.searchsorted(jnp.cumsum(sizes), jnp.arange(rows * top), side="right").astype(jnp.int32)
    listing = items.reshape(top, rows).T
    listing = listing[jax.random.permutation(jax.random.fold_in(own, 1), rows)]
    rotation = jax.random.randint(jax.random.fold_in(own, 2), (rows, 1), 0, top)
    return jnp.take_along_axis(listing, (jnp.arange(top)[None, :] + rotation) % top, axis=1)


def portions_of(number_of, total, reach, skew, full):
    weights = [(1 << 20) // math.isqrt(grade ** skew) + 1 for grade in range(1, number_of + 1)]
    largest = reach if full else min(reach, max(-(-total // number_of), total * weights[0] // sum(weights)))
    least = 1 if total - largest >= number_of - 1 else 0
    holding, surplus = [largest] + [least] * (number_of - 1), total - largest - least * (number_of - 1)
    while surplus > 0:
        candidates = [i for i in range(1, number_of) if holding[i] < largest] or [i for i in range(1, number_of) if holding[i] < reach]
        whole, remaining = sum([weights[i] for i in candidates]), surplus
        for i in candidates:
            extra = min(reach - holding[i], max(1, remaining * weights[i] // whole), surplus)
            holding[i] = holding[i] + extra
            surplus = surplus - extra
    return np.array(holding)


def centred(own_key, dims, deviation, most, pieces=(), kind=jnp.bfloat16):
    loudness = level_of(own_key, dims, pieces, -0.22, 0.18) if pieces else 1.0
    drawn = jax.random.normal(own_key, dims, jnp.float32) * deviation * loudness
    return jnp.minimum(jnp.maximum(drawn, -most), most).astype(kind)


def setup_inputs(seed: int = 0) -> dict:
    splits = jax.random.split(jax.random.key(seed), 8)
    tokens = centred(splits[0], (TOKENS, D), 1.0, 6.0, ((0, 32),))
    expert_id_keys = jax.random.split(jax.random.fold_in(splits[1], 1), TOKENS // TOK_DEV)
    expert_id_turns = jax.random.permutation(jax.random.fold_in(splits[1], 3), TOKENS // TOK_DEV)
    expert_id = jax.vmap(lambda own, number: deal_out(jax.random.fold_in(splits[1], 2), own, number, TOK_DEV, EXPERTS, 1, CAP, 2))(expert_id_keys, expert_id_turns).reshape((TOKENS, 1))
    router_prob = jnp.clip(0.1 + 0.9 * jax.random.uniform(splits[2], (TOKENS,), jnp.float32) ** level_of(splits[2], (TOKENS,), ((0, 32),), -0.2, 0.2), 0.1, 1.0)
    keep_mask = set_ends((jax.random.randint(splits[3], (EXPERTS, SOURCES, FF), 0, 4) < 3).astype(jnp.int32), jax.random.fold_in(splits[3], 1), 0, 1)
    w_in = centred(splits[4], (EXPERTS, D, FF), D ** -0.5, 0.1875, ((0, 16),))
    w_out = centred(splits[5], (EXPERTS, FF, D), FF ** -0.5, 0.125, ((0, 16),))
    cotangent = centred(splits[6], (TOKENS, D), 0.1, 0.59765625, ((0, 32),))
    return dict(tokens=tokens, expert_id=expert_id, router_prob=router_prob, keep_mask=keep_mask, w_in=w_in, w_out=w_out, cotangent=cotangent)


KEEP_SCALE = 4.0 / 3.0


def gelu_parts(pre):
    inner = 0.7978845608 * (pre + 0.044715 * pre * pre * pre)
    tanh_v = jnp.tanh(inner)
    value = 0.5 * pre * (1.0 + tanh_v)
    slope = 0.5 * (1.0 + tanh_v) + 0.5 * pre * (1.0 - tanh_v * tanh_v) * 0.7978845608 * (1.0 + 3.0 * 0.044715 * pre * pre)
    return value, slope


def reference(tokens, expert_id, router_prob, keep_mask, w_in, w_out, cotangent):
    ids = expert_id[:, 0].astype(jnp.int32)
    per = ids.reshape(SOURCES, TOK_DEV)
    onehot = (per[:, :, None] == jnp.arange(EXPERTS, dtype=jnp.int32)[None, None, :]).astype(jnp.int32)
    rank = (jnp.sum(jnp.cumsum(onehot, axis=1) * onehot, axis=2) - 1).reshape(TOKENS).astype(jnp.int32)
    source = (jnp.arange(TOKENS, dtype=jnp.int32) // TOK_DEV).astype(jnp.int32)
    place = (ids * (SOURCES * CAP) + source * CAP + rank).astype(jnp.int32)
    table = jnp.full((EXPERTS * SOURCES * CAP,), TOKENS, jnp.int32).at[place].set(jnp.arange(TOKENS, dtype=jnp.int32))
    table = table.reshape(EXPERTS, SOURCES * CAP)
    gated = (router_prob[:, None] * cotangent.astype(jnp.float32)).astype(jnp.bfloat16)
    x_pad = jnp.concatenate([tokens, jnp.zeros((1, D), tokens.dtype)], axis=0)
    g_pad = jnp.concatenate([gated, jnp.zeros((1, D), gated.dtype)], axis=0)

    def one_expert(args):
        index_row, weight_in, weight_out, keep_rows = args
        rows_x = x_pad[index_row]
        rows_g = g_pad[index_row]
        keep_scale = jnp.repeat(keep_rows.astype(jnp.float32) * KEEP_SCALE, CAP, axis=0)
        pre = jnp.dot(rows_x, weight_in, preferred_element_type=jnp.float32)
        value, slope = gelu_parts(pre)
        hidden = (value * keep_scale).astype(jnp.bfloat16)
        out = jnp.dot(hidden, weight_out, preferred_element_type=jnp.float32).astype(jnp.bfloat16)
        g_out = jnp.dot(hidden.T, rows_g, preferred_element_type=jnp.float32)
        dhidden = jnp.dot(rows_g, weight_out.T, preferred_element_type=jnp.float32)
        dpre = (dhidden * keep_scale * slope).astype(jnp.bfloat16)
        g_in = jnp.dot(rows_x.T, dpre, preferred_element_type=jnp.float32)
        return out, g_in, g_out

    outs, grad_in, grad_out = lax.map(one_expert, (table, w_in, w_out, keep_mask))
    flat = outs.reshape(EXPERTS * SOURCES * CAP, D)
    expert_out = flat[place]
    mixed = (router_prob[:, None] * expert_out.astype(jnp.float32)).astype(jnp.bfloat16)
    return mixed, grad_in, grad_out
```

```python
import jax
import jax.numpy as jnp
from jax import lax
from jax.sharding import PartitionSpec as P

KEEP_SCALE = 4.0 / 3.0


def gelu_parts(pre):
    inner = 0.7978845608 * (pre + 0.044715 * pre * pre * pre)
    tanh_v = jnp.tanh(inner)
    value = 0.5 * pre * (1.0 + tanh_v)
    slope = 0.5 * (1.0 + tanh_v) + 0.5 * pre * (1.0 - tanh_v * tanh_v) * 0.7978845608 * (
        1.0 + 3.0 * 0.044715 * pre * pre
    )
    return (value, slope)


def hidden_parts(received, keep_scale, weight_in):
    sources, slots, width = received.shape
    pre = jnp.dot(
        received.reshape(sources * slots, width), weight_in, preferred_element_type=jnp.float32
    )
    value, slope = gelu_parts(pre)
    value = value.reshape(sources, slots, -1)
    hidden = (value * keep_scale[:, None, :]).astype(jnp.bfloat16)
    return (hidden, slope.reshape(sources, slots, -1))


def expert_forward(received, keep_scale, weight_in, weight_out):
    sources, slots, width = received.shape
    hidden, slope = hidden_parts(received, keep_scale, weight_in)
    out = jnp.dot(
        hidden.reshape(sources * slots, -1), weight_out, preferred_element_type=jnp.float32
    )
    return (out.astype(jnp.bfloat16).reshape(sources, slots, width), hidden, slope)


def halves_summed(columns, rows):
    n_replica = lax.axis_size("replica")
    mine = lax.axis_index("replica")
    part = columns.shape[1] // n_replica

    def product(owner):
        block = lax.dynamic_slice_in_dim(columns, owner * part, part, axis=1)
        return lax.dot_general(
            block, rows, (((0,), (0,)), ((), ())), preferred_element_type=jnp.float32
        )

    total = None
    for shift in range(1, n_replica):
        ring = [(i, (i + shift) % n_replica) for i in range(n_replica)]
        came = lax.ppermute(product((mine + shift) % n_replica), "replica", ring)
        total = came if total is None else total + came
    own = product(mine)
    return own if total is None else own + total


def copies_backward(received, grad_rows, hidden, slope, keep_scale, weight_out):
    sources, slots, width = received.shape
    hidden_width = weight_out.shape[0]
    rows_x = received.reshape(sources * slots, width)
    rows_g = grad_rows.reshape(sources * slots, width)
    flat_hidden = hidden.reshape(sources * slots, hidden_width)
    dhidden = lax.dot_general(
        rows_g, weight_out, (((1,), (1,)), ((), ())), preferred_element_type=jnp.float32
    )
    dpre = (dhidden.reshape(sources, slots, hidden_width) * keep_scale[:, None, :] * slope).astype(
        jnp.bfloat16
    )
    dpre = dpre.reshape(sources * slots, hidden_width)
    grad_out = halves_summed(flat_hidden, rows_g)
    grad_in = halves_summed(rows_x, dpre)
    return (grad_in, grad_out)


def shards(tokens, expert_id, router_prob, keep_mask, w_in, w_out, cotangent):
    tok_rows, width = tokens.shape
    n_expert = lax.axis_size("expert")
    n_replica = lax.axis_size("replica")
    capacity = 2 * tok_rows // n_expert
    portion = capacity // n_replica
    weight_in = w_in[0]
    weight_out = w_out[0]
    ids = expert_id[:, 0]
    onehot = (ids[:, None] == jnp.arange(n_expert, dtype=jnp.int32)[None, :]).astype(jnp.int32)
    ranks = jnp.sum(jnp.cumsum(onehot, axis=0) * onehot, axis=1) - 1
    target = ids * capacity + ranks % n_replica * portion + ranks // n_replica

    def fill_slots(values):
        return jnp.zeros((n_expert * capacity, width), values.dtype).at[target].set(values)

    sent = fill_slots(tokens)
    gated = (router_prob[:, None] * cotangent.astype(jnp.float32)).astype(jnp.bfloat16)
    sent_grad = fill_slots(gated)
    keep_rows = lax.dynamic_index_in_dim(
        keep_mask[0].reshape(n_expert, n_replica, -1),
        lax.axis_index("replica"),
        axis=1,
        keepdims=False,
    )
    keep_scale = keep_rows.astype(jnp.float32) * KEEP_SCALE
    received = lax.all_to_all(
        sent.reshape(n_expert, capacity, width), "expert", split_axis=0, concat_axis=0, tiled=True
    )
    out, hidden, slope = expert_forward(received, keep_scale, weight_in, weight_out)
    grad_rows = lax.all_to_all(
        sent_grad.reshape(n_expert, capacity, width),
        "expert",
        split_axis=0,
        concat_axis=0,
        tiled=True,
    )
    out, hidden, slope, grad_rows = lax.optimization_barrier((out, hidden, slope, grad_rows))
    returned = lax.all_to_all(out, "expert", split_axis=0, concat_axis=0, tiled=True)
    grad_in, grad_out = copies_backward(received, grad_rows, hidden, slope, keep_scale, weight_out)
    returned, grad_in, grad_out = lax.optimization_barrier((returned, grad_in, grad_out))
    expert_out = returned.reshape(n_expert * capacity, width)[target]
    mixed = (router_prob[:, None] * expert_out.astype(jnp.float32)).astype(jnp.bfloat16)
    return (mixed, grad_in[None], grad_out[None])


def solution(mesh):
    in_specs = (
        P(("expert", "replica"), None),
        P(("expert", "replica"), None),
        P(("expert", "replica")),
        P("expert", None, None),
        P("expert", None, None),
        P("expert", None, None),
        P(("expert", "replica"), None),
    )
    out_specs = (
        P(("expert", "replica"), None),
        P("expert", "replica", None),
        P("expert", "replica", None),
    )
    return jax.shard_map(shards, mesh=mesh, in_specs=in_specs, out_specs=out_specs, check_vma=False)
```

```python
import functools

import jax
import jax.numpy as jnp
from jax import lax
from jax.experimental import pallas as pl
from jax.experimental.pallas import tpu as pltpu
from jax.sharding import PartitionSpec as P

KEEP_SCALE = 4.0 / 3.0
MESH = pl.DeviceIdType.MESH


def gelu_parts(pre):
    inner = 0.7978845608 * (pre + 0.044715 * pre * pre * pre)
    tanh_v = jnp.tanh(inner)
    value = 0.5 * pre * (1.0 + tanh_v)
    slope = 0.5 * (1.0 + tanh_v) + 0.5 * pre * (1.0 - tanh_v * tanh_v) * 0.7978845608 * (
        1.0 + 3.0 * 0.044715 * pre * pre
    )
    return (value, slope)


def tile_of(size, most):
    return size if size <= most else most


def kernel(
    n, group,
    sent, sent_grad, keep, w_in, w_out,
    back, grad_in, grad_out,
    weight_in, weight_out, rows_x, rows_g, rows_o, hidden, factor, dpre,
    give_out, came_out, give_in, came_in,
    weight_sem, own_sem, x_send, x_recv, g_send, g_recv, o_send, o_recv, pair_send, pair_recv, done_sem,
):
    me = lax.axis_index("expert")
    core = lax.axis_index("replica")
    other = 1 - core
    cap, width = rows_x.shape[1:]
    ff = weight_in.shape[1]
    rows = group * cap
    groups = n // group
    tile = tile_of(ff, 512)
    wide = tile_of(width, 256)

    def weight_copy(i):
        source, target = ((w_in, weight_in), (w_out, weight_out))[i]
        return pltpu.make_async_copy(source, target, weight_sem.at[i])

    weight_copy(0).start()
    weight_copy(1).start()

    def own_copy(i):
        source, target = (
            (sent.at[me], rows_x.at[0]), (sent_grad.at[me], rows_g.at[0]), (rows_o.at[0], back.at[me])
        )[i]
        return pltpu.make_async_copy(source, target, own_sem.at[i])

    def ahead(k):
        return lax.rem(me + k, n)

    def behind(k):
        return lax.rem(me - k + n, n)

    def x_copy(k):
        return pltpu.make_async_remote_copy(
            src_ref=sent.at[ahead(k)], dst_ref=rows_x.at[k], send_sem=x_send.at[k],
            recv_sem=x_recv.at[k], device_id=(ahead(k), core), device_id_type=MESH,
        )

    def g_copy(k):
        return pltpu.make_async_remote_copy(
            src_ref=sent_grad.at[ahead(k)], dst_ref=rows_g.at[k], send_sem=g_send.at[k],
            recv_sem=g_recv.at[k], device_id=(ahead(k), core), device_id_type=MESH,
        )

    def o_copy(k):
        return pltpu.make_async_remote_copy(
            src_ref=rows_o.at[k], dst_ref=back.at[me], send_sem=o_send.at[k],
            recv_sem=o_recv.at[k], device_id=(behind(k), core), device_id_type=MESH,
        )

    def pair_copy(i):
        source, target = ((give_out, came_out), (give_in, came_in))[i]
        return pltpu.make_async_remote_copy(
            src_ref=source, dst_ref=target, send_sem=pair_send.at[i],
            recv_sem=pair_recv.at[i], device_id=(me, other), device_id_type=MESH,
        )

    def result_copy(i):
        source, target = ((came_out, grad_out), (came_in, grad_in))[i]
        return pltpu.make_async_copy(source, target, done_sem.at[i])

    def each(low, high, step):
        def run(i, carry):
            step(i)
            return carry

        lax.fori_loop(low, high, run, 0)

    own_copy(0).start()
    own_copy(1).start()
    barrier = pltpu.get_barrier_semaphore()

    def greet(k):
        pl.semaphore_signal(barrier, inc=1, device_id=(ahead(k), core), device_id_type=MESH)

    each(1, n, greet)
    pl.semaphore_signal(barrier, inc=1, device_id=(me, other), device_id_type=MESH)
    pl.semaphore_wait(barrier, n)

    each(1, n, lambda k: x_copy(k).start())
    each(1, n, lambda k: g_copy(k).start())
    own_copy(0).wait()
    own_copy(1).wait()
    weight_copy(0).wait()
    weight_copy(1).wait()

    def forward(g):
        first = g * group

        def arrived(k):
            @pl.when(k > 0)
            def _():
                x_copy(k).wait_recv()

        each(first, first + group, arrived)

        def project(j):
            columns = pl.ds(pl.multiple_of(j * tile, tile), tile)
            block = rows_x[pl.ds(first, group)].reshape(rows, width)
            pre = jnp.dot(block, weight_in[:, columns], preferred_element_type=jnp.float32)
            value, slope = gelu_parts(pre)
            scale = keep[pl.ds(first, group), :, columns]
            value = value.reshape(group, cap, tile) * scale
            slope = slope.reshape(group, cap, tile) * scale
            hidden[pl.ds(first, group), :, columns] = value.astype(jnp.bfloat16)
            factor[pl.ds(first, group), :, columns] = slope

        each(0, ff // tile, project)

        def output(j):
            columns = pl.ds(pl.multiple_of(j * wide, wide), wide)
            block = hidden[pl.ds(first, group)].reshape(rows, ff)
            out = jnp.dot(block, weight_out[:, columns], preferred_element_type=jnp.float32)
            rows_o[pl.ds(first, group), :, columns] = out.astype(jnp.bfloat16).reshape(group, cap, wide)

        each(0, width // wide, output)

        def give_back(k):
            @pl.when(k > 0)
            def _():
                o_copy(k).start()

            @pl.when(k == 0)
            def _():
                own_copy(2).start()

        each(first, first + group, give_back)

    each(0, groups, forward)

    def backward(g):
        first = g * group

        def arrived(k):
            @pl.when(k > 0)
            def _():
                g_copy(k).wait_recv()

        each(first, first + group, arrived)

        def pull(j):
            columns = pl.ds(pl.multiple_of(j * tile, tile), tile)
            block = rows_g[pl.ds(first, group)].reshape(rows, width)
            dhidden = lax.dot_general(
                block, weight_out[columns, :], (((1,), (1,)), ((), ())),
                preferred_element_type=jnp.float32,
            )
            dhidden = dhidden.reshape(group, cap, tile) * factor[pl.ds(first, group), :, columns]
            dpre[pl.ds(first, group), :, columns] = dhidden.astype(jnp.bfloat16)

        each(0, ff // tile, pull)

    each(0, groups, backward)

    def product(left, right, start, j, part):
        columns = pl.ds(pl.multiple_of(start + j * part, part), part)
        return lax.dot_general(
            left[:, :, columns].reshape(n * cap, part), right[...].reshape(n * cap, right.shape[2]),
            (((0,), (0,)), ((), ())), preferred_element_type=jnp.float32,
        )

    def gradient(i, left, right, give, came):
        half = give.shape[0]
        part = tile_of(half, 128)

        def theirs(j):
            give[pl.ds(pl.multiple_of(j * part, part), part), :] = product(
                left, right, other * half, j, part)

        def mine(j):
            spot = pl.ds(pl.multiple_of(j * part, part), part)
            came[spot, :] += product(left, right, core * half, j, part)

        return functools.partial(each, 0, half // part, theirs), functools.partial(each, 0, half // part, mine)

    theirs_out, mine_out = gradient(0, hidden, rows_g, give_out, came_out)
    theirs_in, mine_in = gradient(1, rows_x, dpre, give_in, came_in)
    theirs_out()
    pair_copy(0).start()
    theirs_in()
    pair_copy(1).start()
    pair_copy(0).wait_recv()
    mine_out()
    result_copy(0).start()
    pair_copy(1).wait_recv()
    mine_in()
    result_copy(1).start()

    own_copy(2).wait()

    def finish(k):
        x_copy(k).wait_send()
        g_copy(k).wait_send()
        o_copy(k).wait_send()
        o_copy(k).wait_recv()

    each(1, n, finish)
    pair_copy(0).wait_send()
    pair_copy(1).wait_send()
    result_copy(0).wait()
    result_copy(1).wait()


def exchange(sent, sent_grad, keep, w_in, w_out):
    n, cap, width = sent.shape
    ff = w_in.shape[1]
    group = min(n, max(1, 256 // cap))
    dma = pltpu.SemaphoreType.DMA
    f32, bf16 = jnp.float32, jnp.bfloat16
    whole = pl.BlockSpec(memory_space=pl.ANY)
    flops = 10 * n * cap * width * ff
    return pl.pallas_call(
        functools.partial(kernel, n, group),
        out_shape=(
            jax.ShapeDtypeStruct((n, cap, width), bf16),
            jax.ShapeDtypeStruct((width // 2, ff), f32),
            jax.ShapeDtypeStruct((ff // 2, width), f32),
        ),
        in_specs=[whole, whole, pl.BlockSpec(memory_space=pltpu.VMEM), whole, whole],
        out_specs=(whole, whole, whole),
        scratch_shapes=[
            pltpu.VMEM((width, ff), bf16),
            pltpu.VMEM((ff, width), bf16),
            pltpu.VMEM((n, cap, width), bf16),
            pltpu.VMEM((n, cap, width), bf16),
            pltpu.VMEM((n, cap, width), bf16),
            pltpu.VMEM((n, cap, ff), bf16),
            pltpu.VMEM((n, cap, ff), f32),
            pltpu.VMEM((n, cap, ff), bf16),
            pltpu.VMEM((ff // 2, width), f32),
            pltpu.VMEM((ff // 2, width), f32),
            pltpu.VMEM((width // 2, ff), f32),
            pltpu.VMEM((width // 2, ff), f32),
            dma((2,)), dma((3,)), dma((n,)), dma((n,)), dma((n,)), dma((n,)), dma((n,)), dma((n,)),
            dma((2,)), dma((2,)), dma((2,)),
        ],
        cost_estimate=pl.CostEstimate(flops=flops, bytes_accessed=40 << 20, transcendentals=n * cap * ff),
        compiler_params=pltpu.CompilerParams(
            collective_id=0, has_side_effects=True, vmem_limit_bytes=60 << 20
        ),
    )(sent, sent_grad, keep, w_in, w_out)


def shards(tokens, expert_id, router_prob, keep_mask, w_in, w_out, cotangent):
    tok_rows, width = tokens.shape
    n_expert = lax.axis_size("expert")
    n_replica = lax.axis_size("replica")
    capacity = 2 * tok_rows // n_expert
    portion = capacity // n_replica
    weight_in = w_in[0]
    weight_out = w_out[0]
    ids = expert_id[:, 0]
    onehot = (ids[:, None] == jnp.arange(n_expert, dtype=jnp.int32)[None, :]).astype(jnp.int32)
    ranks = jnp.sum(jnp.cumsum(onehot, axis=0) * onehot, axis=1) - 1
    target = ids * capacity + ranks % n_replica * portion + ranks // n_replica

    def fill_slots(values):
        return jnp.zeros((n_expert * capacity, width), values.dtype).at[target].set(values)

    sent = fill_slots(tokens)
    gated = (router_prob[:, None] * cotangent.astype(jnp.float32)).astype(jnp.bfloat16)
    sent_grad = fill_slots(gated)
    keep_rows = lax.dynamic_index_in_dim(
        keep_mask[0].reshape(n_expert, n_replica, -1),
        lax.axis_index("replica"),
        axis=1,
        keepdims=False,
    )
    keep_scale = keep_rows.astype(jnp.float32) * KEEP_SCALE
    sources = (lax.axis_index("expert") - jnp.arange(n_expert) + n_expert) % n_expert
    keep_scale = keep_scale[sources][:, None, :]
    returned, grad_in, grad_out = exchange(
        sent.reshape(n_expert, capacity, width),
        sent_grad.reshape(n_expert, capacity, width),
        keep_scale,
        weight_in,
        weight_out,
    )
    expert_out = returned.reshape(n_expert * capacity, width)[target]
    mixed = (router_prob[:, None] * expert_out.astype(jnp.float32)).astype(jnp.bfloat16)
    return (mixed, grad_in[None], grad_out[None])


def solution(mesh):
    in_specs = (
        P(("expert", "replica"), None),
        P(("expert", "replica"), None),
        P(("expert", "replica")),
        P("expert", None, None),
        P("expert", None, None),
        P("expert", None, None),
        P(("expert", "replica"), None),
    )
    out_specs = (
        P(("expert", "replica"), None),
        P("expert", "replica", None),
        P("expert", "replica", None),
    )
    return jax.shard_map(shards, mesh=mesh, in_specs=in_specs, out_specs=out_specs, check_vma=False)
```

```python
import functools

import jax
import jax.numpy as jnp
from jax import lax
from jax.experimental import pallas as pl
from jax.experimental.pallas import tpu as pltpu
from jax.sharding import PartitionSpec as P

KEEP_SCALE = 4.0 / 3.0
MESH = pl.DeviceIdType.MESH


def gelu_parts(pre):
    inner = 0.7978845608 * (pre + 0.044715 * pre * pre * pre)
    tanh_v = jnp.tanh(inner)
    value = 0.5 * pre * (1.0 + tanh_v)
    slope = 0.5 * (1.0 + tanh_v) + 0.5 * pre * (1.0 - tanh_v * tanh_v) * 0.7978845608 * (
        1.0 + 3.0 * 0.044715 * pre * pre
    )
    return (value, slope)


def tile_of(size, most):
    return size if size <= most else most


def kernel(
    n, group,
    tokens, cotangent, prob, slot_row, slot_column, keep, w_in, w_out,
    mixed, grad_in, grad_out,
    sent, sent_grad, back,
    weight_in, weight_out, rows_x, rows_g, rows_o, hidden, factor, dpre,
    give_out, came_out, came_in,
    weight_sem, own_sem, x_send, x_recv, g_send, g_recv, o_send, o_recv, pair_send, pair_recv, done_sem,
):
    me = lax.axis_index("expert")
    core = lax.axis_index("replica")
    other = 1 - core
    cap, width = rows_x.shape[1:]
    ff = weight_in.shape[1]
    rows = group * cap
    groups = n // group
    tile = tile_of(ff, 512)
    wide = tile_of(width, 256)
    count = tokens.shape[0]
    give_in = factor.at[pl.ds(0, came_in.shape[0])]

    def weight_copy(i):
        source, target = ((w_in, weight_in), (w_out, weight_out))[i]
        return pltpu.make_async_copy(source, target, weight_sem.at[i])

    weight_copy(0).start()
    weight_copy(1).start()

    def own_copy(i):
        source, target = (
            (sent.at[0], rows_x.at[0]), (sent_grad.at[0], rows_g.at[0]), (rows_o.at[0], back.at[me])
        )[i]
        return pltpu.make_async_copy(source, target, own_sem.at[i])

    def ahead(k):
        return lax.rem(me + k, n)

    def behind(k):
        return lax.rem(me - k + n, n)

    def x_copy(k):
        return pltpu.make_async_remote_copy(
            src_ref=sent.at[k], dst_ref=rows_x.at[k], send_sem=x_send.at[k],
            recv_sem=x_recv.at[k], device_id=(ahead(k), core), device_id_type=MESH,
        )

    def g_copy(k):
        return pltpu.make_async_remote_copy(
            src_ref=sent_grad.at[k], dst_ref=rows_g.at[k], send_sem=g_send.at[k],
            recv_sem=g_recv.at[k], device_id=(ahead(k), core), device_id_type=MESH,
        )

    def o_copy(k):
        return pltpu.make_async_remote_copy(
            src_ref=rows_o.at[k], dst_ref=back.at[me], send_sem=o_send.at[k],
            recv_sem=o_recv.at[k], device_id=(behind(k), core), device_id_type=MESH,
        )

    def pair_copy(i):
        source, target = ((give_out, came_out), (give_in, came_in))[i]
        return pltpu.make_async_remote_copy(
            src_ref=source, dst_ref=target, send_sem=pair_send.at[i],
            recv_sem=pair_recv.at[i], device_id=(me, other), device_id_type=MESH,
        )

    def result_copy(i):
        source, target = ((came_out, grad_out), (came_in, grad_in))[i]
        return pltpu.make_async_copy(source, target, done_sem.at[i])

    def each(low, high, step):
        def run(i, carry):
            step(i)
            return carry

        lax.fori_loop(low, high, run, 0)

    barrier = pltpu.get_barrier_semaphore()

    def greet(k):
        pl.semaphore_signal(barrier, inc=1, device_id=(ahead(k), core), device_id_type=MESH)

    each(1, n, greet)
    pl.semaphore_signal(barrier, inc=1, device_id=(me, other), device_id_type=MESH)

    def dispatch(values, slots):
        def fill(g):
            first = g * group
            shape = (group, cap, count)
            expert = lax.broadcasted_iota(jnp.int32, shape, 0) + (first + me)
            expert = jnp.where(expert >= n, expert - n, expert)
            place = expert * cap + lax.broadcasted_iota(jnp.int32, shape, 1)
            chosen = jnp.where(place == slot_row[...][None], 1.0, 0.0).astype(jnp.bfloat16)
            filled = jnp.dot(
                chosen.reshape(rows, count), values[...], preferred_element_type=jnp.float32
            )
            slots[pl.ds(first, group)] = filled.astype(jnp.bfloat16).reshape(group, cap, width)

        each(0, groups, fill)

    def later(copy):
        def start(i):
            k = lax.rem((1 - core) * (i + n // 4) + core * (n // 4 * 3 - 1 - i + n), n)

            @pl.when(k > 0)
            def _():
                copy(k).start()

        return start

    dispatch(tokens, sent)
    own_copy(0).start()
    pl.semaphore_wait(barrier, n)
    each(0, n, later(x_copy))
    mixed[...] = (prob[...] * cotangent[...].astype(jnp.float32)).astype(jnp.bfloat16)
    dispatch(mixed, sent_grad)
    own_copy(1).start()
    each(0, n, later(g_copy))
    own_copy(0).wait()
    own_copy(1).wait()
    weight_copy(0).wait()
    weight_copy(1).wait()

    def span(first):
        return pl.ds(pl.multiple_of(first * cap, rows), rows)

    def forward(g):
        first = lax.rem((1 - core) * (g + groups // 4) + core * (groups // 4 * 3 - 1 - g + groups), groups) * group

        def arrived(k):
            @pl.when(k > 0)
            def _():
                x_copy(k).wait_recv()

        each(first, first + group, arrived)

        def project(j):
            columns = pl.ds(pl.multiple_of(j * tile, tile), tile)
            block = rows_x[pl.ds(first, group)].reshape(rows, width)
            pre = jnp.dot(block, weight_in[:, columns], preferred_element_type=jnp.float32)
            value, slope = gelu_parts(pre)
            scale = keep[pl.ds(first, group), :, columns]
            value = value.reshape(group, cap, tile) * scale
            slope = slope.reshape(group, cap, tile) * scale
            hidden[pl.ds(first, group), :, columns] = value.astype(jnp.bfloat16)
            factor[span(first), columns] = slope.reshape(rows, tile)

        each(0, ff // tile, project)

        def output(j):
            columns = pl.ds(pl.multiple_of(j * wide, wide), wide)
            block = hidden[pl.ds(first, group)].reshape(rows, ff)
            out = jnp.dot(block, weight_out[:, columns], preferred_element_type=jnp.float32)
            rows_o[pl.ds(first, group), :, columns] = out.astype(jnp.bfloat16).reshape(group, cap, wide)

        each(0, width // wide, output)

        def give_back(k):
            @pl.when(k > 0)
            def _():
                o_copy(k).start()

            @pl.when(k == 0)
            def _():
                own_copy(2).start()

        each(first, first + group, give_back)

    each(0, groups, forward)

    def backward(g):
        first = lax.rem((1 - core) * (g + groups // 4) + core * (groups // 4 * 3 - 1 - g + groups), groups) * group

        def arrived(k):
            @pl.when(k > 0)
            def _():
                g_copy(k).wait_recv()

        each(first, first + group, arrived)

        def pull(j):
            columns = pl.ds(pl.multiple_of(j * tile, tile), tile)
            block = rows_g[pl.ds(first, group)].reshape(rows, width)
            dhidden = lax.dot_general(
                block, weight_out[columns, :], (((1,), (1,)), ((), ())),
                preferred_element_type=jnp.float32,
            )
            dhidden = (dhidden * factor[span(first), columns]).astype(jnp.bfloat16)
            dpre[pl.ds(first, group), :, columns] = dhidden.reshape(group, cap, tile)

        each(0, ff // tile, pull)

    each(0, groups, backward)

    def product(left, right, start, j, part):
        columns = pl.ds(pl.multiple_of(start + j * part, part), part)
        return lax.dot_general(
            left[:, :, columns].reshape(n * cap, part), right[...].reshape(n * cap, right.shape[2]),
            (((0,), (0,)), ((), ())), preferred_element_type=jnp.float32,
        )

    def gradient(i, left, right, give, came):
        half = give.shape[0]
        part = tile_of(half, 256)

        def theirs(j):
            give[pl.ds(pl.multiple_of(j * part, part), part), :] = product(
                left, right, other * half, j, part)

        def mine(j):
            spot = pl.ds(pl.multiple_of(j * part, part), part)
            came[spot, :] += product(left, right, core * half, j, part)

        return functools.partial(each, 0, half // part, theirs), functools.partial(each, 0, half // part, mine)

    theirs_out, mine_out = gradient(0, hidden, rows_g, give_out, came_out)
    theirs_in, mine_in = gradient(1, rows_x, dpre, give_in, came_in)
    theirs_out()
    pair_copy(0).start()
    theirs_in()
    pair_copy(1).start()
    pair_copy(0).wait_recv()
    mine_out()
    result_copy(0).start()
    pair_copy(1).wait_recv()
    mine_in()
    result_copy(1).start()

    own_copy(2).wait()

    def finish(k):
        x_copy(k).wait_send()
        g_copy(k).wait_send()
        o_copy(k).wait_send()

    each(1, n, lambda k: o_copy(k).wait_recv())

    def combine(j):
        columns = pl.ds(pl.multiple_of(j * wide, wide), wide)
        place = lax.broadcasted_iota(jnp.int32, (count, n * cap), 1)
        chosen = jnp.where(place == slot_column[...], 1.0, 0.0).astype(jnp.bfloat16)
        out = jnp.dot(
            chosen, back[:, :, columns].reshape(n * cap, wide), preferred_element_type=jnp.float32
        )
        mixed[:, columns] = (prob[...] * out).astype(jnp.bfloat16)

    each(0, width // wide, combine)
    each(1, n, finish)
    pair_copy(0).wait_send()
    pair_copy(1).wait_send()
    result_copy(0).wait()
    result_copy(1).wait()


def exchange(n, cap, tokens, cotangent, prob, target, keep, w_in, w_out):
    count, width = tokens.shape
    ff = w_in.shape[1]
    group = min(n, max(1, 256 // cap))
    dma = pltpu.SemaphoreType.DMA
    f32, bf16 = jnp.float32, jnp.bfloat16
    whole = pl.BlockSpec(memory_space=pl.ANY)
    flops = 10 * n * cap * width * ff
    return pl.pallas_call(
        functools.partial(kernel, n, group),
        out_shape=(
            jax.ShapeDtypeStruct((count, width), bf16),
            jax.ShapeDtypeStruct((width // 2, ff), f32),
            jax.ShapeDtypeStruct((ff // 2, width), f32),
        ),
        in_specs=[pl.BlockSpec(memory_space=pltpu.VMEM)] * 6 + [whole, whole],
        out_specs=(pl.BlockSpec(memory_space=pltpu.VMEM), whole, whole),
        scratch_shapes=[
            pltpu.VMEM((n, cap, width), bf16),
            pltpu.VMEM((n, cap, width), bf16),
            pltpu.VMEM((n, cap, width), bf16),
            pltpu.VMEM((width, ff), bf16),
            pltpu.VMEM((ff, width), bf16),
            pltpu.VMEM((n, cap, width), bf16),
            pltpu.VMEM((n, cap, width), bf16),
            pltpu.VMEM((n, cap, width), bf16),
            pltpu.VMEM((n, cap, ff), bf16),
            pltpu.VMEM((n * cap, ff), f32),
            pltpu.VMEM((n, cap, ff), bf16),
            pltpu.VMEM((ff // 2, width), f32),
            pltpu.VMEM((ff // 2, width), f32),
            pltpu.VMEM((width // 2, ff), f32),
            dma((2,)), dma((3,)), dma((n,)), dma((n,)), dma((n,)), dma((n,)), dma((n,)), dma((n,)),
            dma((2,)), dma((2,)), dma((2,)),
        ],
        cost_estimate=pl.CostEstimate(flops=flops, bytes_accessed=40 << 20, transcendentals=n * cap * ff),
        compiler_params=pltpu.CompilerParams(
            collective_id=0, has_side_effects=True, vmem_limit_bytes=67043328
        ),
    )(tokens, cotangent, prob[:, None], target[None, :], target[:, None], keep, w_in, w_out)


def shards(tokens, expert_id, router_prob, keep_mask, w_in, w_out, cotangent):
    tok_rows, width = tokens.shape
    n_expert = lax.axis_size("expert")
    n_replica = lax.axis_size("replica")
    capacity = 2 * tok_rows // n_expert
    portion = capacity // n_replica
    weight_in = w_in[0]
    weight_out = w_out[0]
    ids = expert_id[:, 0]
    onehot = (ids[:, None] == jnp.arange(n_expert, dtype=jnp.int32)[None, :]).astype(jnp.int32)
    ranks = jnp.sum(jnp.cumsum(onehot, axis=0) * onehot, axis=1) - 1
    target = ids * capacity + ranks % n_replica * portion + ranks // n_replica
    keep_rows = lax.dynamic_index_in_dim(
        keep_mask[0].reshape(n_expert, n_replica, -1),
        lax.axis_index("replica"),
        axis=1,
        keepdims=False,
    )
    keep_scale = keep_rows.astype(jnp.float32) * KEEP_SCALE
    sources = (lax.axis_index("expert") - jnp.arange(n_expert) + n_expert) % n_expert
    keep_scale = keep_scale[sources][:, None, :]
    mixed, grad_in, grad_out = exchange(
        n_expert, capacity, tokens, cotangent, router_prob, target, keep_scale, weight_in, weight_out
    )
    return (mixed, grad_in[None], grad_out[None])


def solution(mesh):
    in_specs = (
        P(("expert", "replica"), None),
        P(("expert", "replica"), None),
        P(("expert", "replica")),
        P("expert", None, None),
        P("expert", None, None),
        P("expert", None, None),
        P(("expert", "replica"), None),
    )
    out_specs = (
        P(("expert", "replica"), None),
        P("expert", "replica", None),
        P("expert", "replica", None),
    )
    return jax.shard_map(shards, mesh=mesh, in_specs=in_specs, out_specs=out_specs, check_vma=False)
```
